32 devices in a mesh: row: 4 (over z), col: 2 (over y), depth: 4 (over x, core).
Axes of the slice: x: 2, y: 2, z: 4, core: 2. Of those that a mesh axis runs over, the one named last changes fastest.
Arguments:
- factor: float32 [4096, 1536], P(('row', 'col', 'depth')), may hold values from -1 to 4, as said below
- update: float32 [4096, 256], P(('row', 'col', 'depth')), may hold values from -0.375 to 0.375
Outputs:
- new_factor: float32 [4096, 1536], P(('row', 'col', 'depth'))
- new_update: float32 [4096, 256], P(('row', 'col', 'depth'))
The draws below stay inside these ranges and needn't reach their ends.
Inputs may be any that keep to these rules, and one draw needn't show every extreme that they name: `factor`: zero above the diagonal; each diagonal entry is 1 or more.
All inputs are finite; a program needn't handle non-finite values.
Results may differ from the reference program's by a relative error of at most 0.00013.
Values sent between devices are 32-bit elements; how exact they have to be, the bound alone decides.
A program may use at most 128 MiB of HBM per device.

```python
import math
import jax
import jax.numpy as jnp
from jax import lax

B = 512
K = 256
PANELS = 3
N = 4096
WIN = 1536


def draw_factor(key, part):
    key_off, key_diag = jax.random.split(key)
    row_ids = jnp.arange(N, dtype=jnp.int32)[:, None]
    col_ids = jnp.arange(WIN, dtype=jnp.int32)[None, :]
    lower_part = jax.random.normal(key_off, (N, WIN), jnp.float32) / math.sqrt(B)
    diagonal = jax.random.uniform(key_diag, (WIN,), jnp.float32, 1.0, 2.0)
    lower_part = jnp.clip(lower_part, -0.9, 0.9)
    return jnp.where(row_ids > col_ids, lower_part, jnp.where(row_ids == col_ids, diagonal[None, :], jnp.float32(0.0)))


def level_of(own_key, shape, pieces, least, high):
    level, own = 1.0, jax.random.fold_in(own_key, 6)
    for position, blocks in pieces:
        steps = jnp.exp(jax.random.uniform(jax.random.fold_in(own, position), (blocks,), jnp.float32, least / len(pieces), high / len(pieces)))
        level = level * jnp.repeat(steps, shape[position] // blocks).reshape([-1 if axis == position else 1 for axis in range(len(shape))])
    return level


def noise(key, dims, scale, most, cuts=(), kind=jnp.bfloat16):
    loudness = level_of(key, dims, cuts, -0.22, 0.18) if cuts else 1.0
    drawn = jax.random.normal(key, dims, jnp.float32) * scale * loudness
    return jnp.minimum(jnp.maximum(drawn, -most), most).astype(kind)


def setup_inputs(seed: int = 0) -> dict:
    streams_of = jax.random.split(jax.random.key(seed), 3)
    factor = draw_factor(jax.random.fold_in(streams_of[2], 71), 0)
    update = noise(streams_of[1], (N, K), 0.0625, 0.375, ((0, 32),), jnp.float32)
    return dict(factor=factor, update=update)


def transform(stacked):
    panel_width = stacked.shape[0]
    diag_block = stacked[:, :panel_width]
    v_block = stacked[:, panel_width:]
    update_rank = v_block.shape[1]
    gram_matrix = jnp.dot(stacked, stacked.T, precision=lax.Precision.HIGHEST)
    new_diag = jnp.linalg.cholesky(gram_matrix)
    leading = jax.scipy.linalg.solve_triangular(new_diag, stacked, lower=True)
    coupling = jax.scipy.linalg.solve_triangular(diag_block, v_block, lower=True)
    identity_k = jnp.eye(update_rank, dtype=jnp.float32)
    inner_gram = identity_k + jnp.dot(coupling.T, coupling, precision=lax.Precision.HIGHEST)
    lower_inner = jnp.linalg.cholesky(inner_gram)
    null_basis = jnp.concatenate([-coupling, identity_k], 0)
    second = jax.scipy.linalg.solve_triangular(lower_inner, null_basis.T, lower=True).T
    return jnp.concatenate([leading.T, second], 1)

def reference(factor, update):
    row_ids = jnp.arange(N, dtype=jnp.int32)
    for panel_index in range(PANELS):
        panel_start = panel_index * B
        panel_cols = factor[:, panel_start:panel_start + B]
        stacked = jnp.concatenate([panel_cols, update], 1)
        rotation = transform(stacked[panel_start:panel_start + B])
        moved = jnp.dot(stacked, rotation, precision=lax.Precision.HIGHEST)
        col_ids = panel_start + jnp.arange(B, dtype=jnp.int32)
        new_cols = jnp.where(row_ids[:, None] >= col_ids[None, :], moved[:, :B], jnp.float32(0.0))
        update = jnp.where(row_ids[:, None] >= panel_start, moved[:, B:], update)
        factor = factor.at[:, panel_start:panel_start + B].set(new_cols)
    return (factor, update)
```

```python
import functools

import jax
import jax.numpy as jnp
from jax import lax
from jax.experimental import pallas as pl
from jax.experimental.pallas import tpu as pltpu
from jax.sharding import PartitionSpec as P

B = 512
PANELS = 3
T = 128
S = 16
NN = ((1,), (0,))
NT = ((1,), (1,))
TN = ((0,), (0,))


def split(x):
    high = x.astype(jnp.bfloat16)
    return high, (x - high.astype(jnp.float32)).astype(jnp.bfloat16)


def mms(a, b, dims):
    def dot(p, q):
        return lax.dot_general(p, q, (dims, ((), ())), preferred_element_type=jnp.float32)

    return dot(a[0], b[0]) + (dot(a[0], b[1]) + dot(a[1], b[0]))


def mm(a, b, dims):
    return mms(split(a), split(b), dims)


def invert(ref, count, symmetric):
    sub = lax.broadcasted_iota(jnp.int32, (S, T), 0)
    lane = lax.broadcasted_iota(jnp.int32, (S, T), 1)
    all_lane = lax.broadcasted_iota(jnp.int32, (T, T), 1)
    all_row = lax.broadcasted_iota(jnp.int32, (T, T), 0)

    def body(block, carry):
        first = pl.multiple_of(block * S, S)
        rows = [
            pltpu.roll(ref[m, pl.ds(first, S), :], lax.rem(T - first, T), 1) for m in range(count)
        ]
        diag = [jnp.ones((S, T), jnp.float32) for _ in range(count)]
        for s in range(S):
            for m in range(count):
                r = rows[m]
                col = jnp.broadcast_to(r[:, s : s + 1], (S, T))
                pivot = jnp.broadcast_to(col[s : s + 1, :], (S, T))
                diag[m] = jnp.where(sub == s, pivot, diag[m])
                r = jnp.where((lane == s) & (sub >= s), jnp.where(sub == s, 1.0, 0.0), r)
                scaled = r[s : s + 1, :] / pivot[0:1, :]
                rows[m] = r - jnp.where(sub > s, col, 0.0) * scaled
        in_block = (all_lane >= first) & (all_lane < first + S)
        for m in range(count):
            r = rows[m]
            r = r * lax.rsqrt(diag[m]) if symmetric else r / diag[m]
            r = pltpu.roll(r, first, 1)
            r = jnp.where((lane > sub + first) & (lane < first + S), 0.0, r)
            a = ref[m]
            right = split(r)
            if symmetric:
                left = split(jnp.where(lane >= first + S, r, 0.0))
                change = mms(left, right, TN)
                ref[m] = jnp.where(in_block, 0.0, a) - change
            else:
                left = jnp.where(in_block & (all_row >= first + S), a, 0.0)
                wide = [jnp.where(all_row // S == block, jnp.concatenate([q.astype(jnp.float32)] * (T // S), 0), 0.0).astype(jnp.bfloat16) for q in right]
                change = mms(split(left), wide, NN)
                ref[m] = jnp.where(in_block, 0.0, a) - change
            ref[m, pl.ds(first, S), :] = jnp.where(lane <= sub + first, r, 0.0)
        return carry

    lax.fori_loop(0, T // S, body, 0)


def kernel(start_ref, *refs):
    fs = refs[:PANELS]
    us = refs[PANELS : 2 * PANELS]
    f_ref, u_ref, of_ref, ou_ref = refs[2 * PANELS : 2 * PANELS + 4]
    dinv, w11, w22, w21, tinv_h, tinv_l, sinv, hh, hl, gh, gl = refs[2 * PANELS + 4 :]
    per = B // T
    count = PANELS * per
    rank = u_ref.shape[1]
    half = rank // 2
    eye = jnp.where(
        lax.broadcasted_iota(jnp.int32, (T, T), 0) == lax.broadcasted_iota(jnp.int32, (T, T), 1), 1.0, 0.0
    )

    def blk(j):
        return slice(j * T, (j + 1) * T)

    for j in range(count):
        dinv[j] = fs[j // per][blk(j % per), blk(j)]
    invert(dinv, count, False)

    total = [[eye, None], [jnp.zeros((half, half), jnp.float32), eye]]
    for j in range(count):
        t = us[j // per][blk(j % per), :]
        if j:
            left = split(fs[j // per][blk(j % per), : j * T])
            t = t - mms(left, (hh[: j * T, :], hl[: j * T, :]), NN)
        h = split(mm(dinv[j], t, NN))
        hh[blk(j), :], hl[blk(j), :] = h
        g = mms(h, h, TN)
        total[0][0] = total[0][0] + g[:half, :half]
        total[1][0] = total[1][0] + g[half:, :half]
        total[1][1] = total[1][1] + g[half:, half:]
        w11[j], w21[j], w22[j] = total[0][0], total[1][0], total[1][1]

    invert(w11, count, True)
    for j in range(count):
        low = mm(w21[j], w11[j], NT)
        w21[j] = low
        low = split(low)
        w22[j] = w22[j] - mms(low, low, NT)
    invert(w22, count, True)
    for j in range(count):
        x21 = -mm(w22[j], mm(w21[j], w11[j], NN), NN)
        for out, x11, x2, x22 in zip((tinv_h, tinv_l), split(w11[j]), split(x21), split(w22[j])):
            out[j, :half, :half] = x11
            out[j, :half, half:] = jnp.zeros_like(x11)
            out[j, half:, :half] = x2
            out[j, half:, half:] = x22
    for j in range(count):
        h = (hh[blk(j), :], hl[blk(j), :])
        g = h if j == 0 else split(mms(h, (tinv_h[j - 1], tinv_l[j - 1]), NT))
        gh[blk(j), :], gl[blk(j), :] = g
        sinv[j] = eye + mms(g, g, NT)
    invert(sinv, count, True)

    rows = f_ref.shape[0]
    row_ids = start_ref[0] + lax.broadcasted_iota(jnp.int32, (rows, T), 0)
    lane = lax.broadcasted_iota(jnp.int32, (rows, T), 1)
    res = u_ref[...]
    for j in range(count):
        f = f_ref[:, blk(j)]
        u = split(res)
        if j:
            u = split(mms(u, (tinv_h[j - 1], tinv_l[j - 1]), NT))
        z = f + mms(u, (gh[blk(j), :], gl[blk(j), :]), NT)
        y = mm(z, sinv[j], NT)
        of_ref[:, blk(j)] = jnp.where(row_ids >= lane + j * T, y, 0.0)
        res = res - mms(split(f), (hh[blk(j), :], hl[blk(j), :]), NN)
    last = start_ref[1]
    ou_ref[...] = mms(split(res), (tinv_h[last], tinv_l[last]), NT)


def update_rows(start, slabs, updates, factor, update):
    count = PANELS * B // T
    rank = update.shape[1]
    half = rank // 2
    f32, b16 = jnp.float32, jnp.bfloat16
    vmem = pl.BlockSpec(memory_space=pltpu.VMEM)
    return pl.pallas_call(
        kernel,
        out_shape=(
            jax.ShapeDtypeStruct(factor.shape, f32),
            jax.ShapeDtypeStruct(update.shape, f32),
        ),
        in_specs=[pl.BlockSpec(memory_space=pltpu.SMEM)] + [vmem] * (2 * PANELS + 2),
        out_specs=(vmem, vmem),
        scratch_shapes=[
            pltpu.VMEM((count, T, T), f32),
            pltpu.VMEM((count, half, half), f32),
            pltpu.VMEM((count, half, half), f32),
            pltpu.VMEM((count, half, half), f32),
            pltpu.VMEM((count, rank, rank), b16),
            pltpu.VMEM((count, rank, rank), b16),
            pltpu.VMEM((count, T, T), f32),
            pltpu.VMEM((count * T, rank), b16),
            pltpu.VMEM((count * T, rank), b16),
            pltpu.VMEM((count * T, rank), b16),
            pltpu.VMEM((count * T, rank), b16),
        ],
        compiler_params=pltpu.CompilerParams(vmem_limit_bytes=56 * 1024 * 1024),
    )(start, *slabs, *updates, factor, update)


def spread(block, axis, owner):
    block = jnp.where(lax.axis_index(axis) == owner, block, jnp.zeros_like(block))
    return lax.psum(block, axis)


def on_device(factor, update):
    rows_dev = factor.shape[0]
    row_start = lax.axis_index(("row", "col", "depth")) * rows_dev
    panel = jnp.minimum(row_start // B, PANELS - 1)
    start = jnp.stack([row_start, (panel + 1) * (B // T) - 1]).astype(jnp.int32)
    slabs, updates = [], []
    for owner in range(PANELS):
        width = (owner + 1) * B
        joined = jnp.concatenate([factor[:, :width], update], 1)
        joined = spread(joined, ("row", "col"), owner)
        joined = lax.all_gather(joined, "depth", axis=0, tiled=True)
        slabs.append(joined[:, :width])
        updates.append(joined[:, width:])
    return update_rows(start, slabs, updates, factor, update)


def solution(mesh):
    return jax.shard_map(
        on_device,
        mesh=mesh,
        in_specs=(P(("row", "col", "depth"), None), P(("row", "col", "depth"), None)),
        out_specs=(P(("row", "col", "depth"), None), P(("row", "col", "depth"), None)),
        check_vma=False,
    )
```

```python
import functools

import jax
import jax.numpy as jnp
from jax import lax
from jax.experimental import pallas as pl
from jax.experimental.pallas import tpu as pltpu
from jax.sharding import PartitionSpec as P

B = 512
PANELS = 3
T = 128
PIECES = 4
MESH = pl.DeviceIdType.MESH
S = 16
NN = ((1,), (0,))
NT = ((1,), (1,))
TN = ((0,), (0,))


def split(x):
    high = x.astype(jnp.bfloat16)
    return high, (x - high.astype(jnp.float32)).astype(jnp.bfloat16)


def mms(a, b, dims):
    def dot(p, q):
        return lax.dot_general(p, q, (dims, ((), ())), preferred_element_type=jnp.float32)

    return dot(a[0], b[0]) + (dot(a[0], b[1]) + dot(a[1], b[0]))


def mm(a, b, dims):
    return mms(split(a), split(b), dims)


def invert(ref, count, symmetric):
    sub = lax.broadcasted_iota(jnp.int32, (S, T), 0)
    lane = lax.broadcasted_iota(jnp.int32, (S, T), 1)
    all_lane = lax.broadcasted_iota(jnp.int32, (T, T), 1)
    all_row = lax.broadcasted_iota(jnp.int32, (T, T), 0)

    def body(block, carry):
        first = pl.multiple_of(block * S, S)
        rows = [
            pltpu.roll(ref[m, pl.ds(first, S), :], lax.rem(T - first, T), 1) for m in range(count)
        ]
        diag = [jnp.ones((S, T), jnp.float32) for _ in range(count)]
        for s in range(S):
            for m in range(count):
                r = rows[m]
                col = jnp.broadcast_to(r[:, s : s + 1], (S, T))
                pivot = jnp.broadcast_to(col[s : s + 1, :], (S, T))
                diag[m] = jnp.where(sub == s, pivot, diag[m])
                r = jnp.where((lane == s) & (sub >= s), jnp.where(sub == s, 1.0, 0.0), r)
                scaled = r[s : s + 1, :] / pivot[0:1, :]
                rows[m] = r - jnp.where(sub > s, col, 0.0) * scaled
        in_block = (all_lane >= first) & (all_lane < first + S)
        for m in range(count):
            r = rows[m]
            r = r * lax.rsqrt(diag[m]) if symmetric else r / diag[m]
            r = pltpu.roll(r, first, 1)
            r = jnp.where((lane > sub + first) & (lane < first + S), 0.0, r)
            a = ref[m]
            right = split(r)
            if symmetric:
                left = split(jnp.where(lane >= first + S, r, 0.0))
                change = mms(left, right, TN)
                ref[m] = jnp.where(in_block, 0.0, a) - change
            else:
                left = jnp.where(in_block & (all_row >= first + S), a, 0.0)
                wide = [jnp.where(all_row // S == block, jnp.concatenate([q.astype(jnp.float32)] * (T // S), 0), 0.0).astype(jnp.bfloat16) for q in right]
                change = mms(split(left), wide, NN)
                ref[m] = jnp.where(in_block, 0.0, a) - change
            ref[m, pl.ds(first, S), :] = jnp.where(lane <= sub + first, r, 0.0)
        return carry

    lax.fori_loop(0, T // S, body, 0)


def kernel(start_ref, *refs):
    xs = refs[:PANELS]
    f_ref, u_ref, of_ref, ou_ref = refs[PANELS : PANELS + 4]
    dinv, w11, w22, w21, tinv_h, tinv_l, sinv, hh, hl, gh, gl = refs[PANELS + 4 :]
    per = B // T
    count = PANELS * per
    rank = u_ref.shape[1]
    half = rank // 2
    eye = jnp.where(
        lax.broadcasted_iota(jnp.int32, (T, T), 0) == lax.broadcasted_iota(jnp.int32, (T, T), 1), 1.0, 0.0
    )

    def blk(j):
        return slice(j * T, (j + 1) * T)

    for j in range(count):
        dinv[j] = xs[j // per][blk(j % per), rank + j * T : rank + (j + 1) * T]
    invert(dinv, count, False)

    total = [[eye, None], [jnp.zeros((half, half), jnp.float32), eye]]
    for j in range(count):
        t = xs[j // per][blk(j % per), :rank]
        if j:
            left = split(xs[j // per][blk(j % per), rank : rank + j * T])
            t = t - mms(left, (hh[: j * T, :], hl[: j * T, :]), NN)
        h = split(mm(dinv[j], t, NN))
        hh[blk(j), :], hl[blk(j), :] = h
        g = mms(h, h, TN)
        total[0][0] = total[0][0] + g[:half, :half]
        total[1][0] = total[1][0] + g[half:, :half]
        total[1][1] = total[1][1] + g[half:, half:]
        w11[j], w21[j], w22[j] = total[0][0], total[1][0], total[1][1]

    invert(w11, count, True)
    for j in range(count):
        low = mm(w21[j], w11[j], NT)
        w21[j] = low
        low = split(low)
        w22[j] = w22[j] - mms(low, low, NT)
    invert(w22, count, True)
    for j in range(count):
        x21 = -mm(w22[j], mm(w21[j], w11[j], NN), NN)
        for out, x11, x2, x22 in zip((tinv_h, tinv_l), split(w11[j]), split(x21), split(w22[j])):
            out[j, :half, :half] = x11
            out[j, :half, half:] = jnp.zeros_like(x11)
            out[j, half:, :half] = x2
            out[j, half:, half:] = x22
    for j in range(count):
        h = (hh[blk(j), :], hl[blk(j), :])
        g = h if j == 0 else split(mms(h, (tinv_h[j - 1], tinv_l[j - 1]), NT))
        gh[blk(j), :], gl[blk(j), :] = g
        sinv[j] = eye + mms(g, g, NT)
    invert(sinv, count, True)

    rows = f_ref.shape[0]
    row_ids = start_ref[0] + lax.broadcasted_iota(jnp.int32, (rows, T), 0)
    lane = lax.broadcasted_iota(jnp.int32, (rows, T), 1)
    res = u_ref[...]
    for j in range(count):
        f = f_ref[:, blk(j)]
        u = split(res)
        if j:
            u = split(mms(u, (tinv_h[j - 1], tinv_l[j - 1]), NT))
        z = f + mms(u, (gh[blk(j), :], gl[blk(j), :]), NT)
        y = mm(z, sinv[j], NT)
        of_ref[:, blk(j)] = jnp.where(row_ids >= lane + j * T, y, 0.0)
        res = res - mms(split(f), (hh[blk(j), :], hl[blk(j), :]), NN)
    last = start_ref[1]
    ou_ref[...] = mms(split(res), (tinv_h[last], tinv_l[last]), NT)


def update_rows(start, slabs, factor, update):
    count = PANELS * B // T
    rank = update.shape[1]
    half = rank // 2
    f32, b16 = jnp.float32, jnp.bfloat16
    vmem = pl.BlockSpec(memory_space=pltpu.VMEM)
    return pl.pallas_call(
        kernel,
        out_shape=(
            jax.ShapeDtypeStruct(factor.shape, f32),
            jax.ShapeDtypeStruct(update.shape, f32),
        ),
        in_specs=[pl.BlockSpec(memory_space=pltpu.SMEM)] + [vmem] * (PANELS + 2),
        out_specs=(vmem, vmem),
        scratch_shapes=[
            pltpu.VMEM((count, T, T), f32),
            pltpu.VMEM((count, half, half), f32),
            pltpu.VMEM((count, half, half), f32),
            pltpu.VMEM((count, half, half), f32),
            pltpu.VMEM((count, rank, rank), b16),
            pltpu.VMEM((count, rank, rank), b16),
            pltpu.VMEM((count, T, T), f32),
            pltpu.VMEM((count * T, rank), b16),
            pltpu.VMEM((count * T, rank), b16),
            pltpu.VMEM((count * T, rank), b16),
            pltpu.VMEM((count * T, rank), b16),
        ],
        compiler_params=pltpu.CompilerParams(vmem_limit_bytes=56 * 1024 * 1024),
    )(start, *slabs, factor, update)


def send_kernel(sizes, x_ref, *refs):
    outs = refs[:PANELS]
    local_sem, col_send, col_recv, row_send, row_recv, depth_send, depth_recv = refs[PANELS:]
    n_row, n_col, n_depth = sizes
    r, c, d = (lax.axis_index(name) for name in ("row", "col", "depth"))
    bits = [1 << b for b in reversed(range(n_depth.bit_length() - 1))]
    rows_dev = x_ref.shape[0]
    piece = rows_dev // PIECES
    barrier = pltpu.get_barrier_semaphore()

    def greet(target):
        pl.semaphore_signal(barrier, inc=1, device_id=target, device_id_type=MESH)

    for k in range(1, n_col):
        greet({"col": lax.rem(c + k, n_col)})
    for bit in bits:
        greet({"depth": d ^ bit})
    turns = (1, n_row - 1) if n_row > 1 else ()
    for k in turns:
        greet({"row": lax.rem(r + k, n_row)})
    pl.semaphore_wait(barrier, n_col - 1 + len(bits) + len(turns))

    def part(p, s, owner):
        return outs[p].at[owner, pl.ds(s * piece, piece), :]

    def remote(ref, send, recv, target):
        return pltpu.make_async_remote_copy(
            src_ref=ref, dst_ref=ref, send_sem=send, recv_sem=recv, device_id=target, device_id_type=MESH
        )

    def local(p, s, q):
        width = outs[p].shape[2]
        return pltpu.make_async_copy(x_ref.at[pl.ds(s * piece, piece), :width], part(p, s, d), local_sem.at[q])

    def col_copy(p, s, q, k):
        return remote(part(p, s, d), col_send.at[q, k], col_recv.at[q], {"col": lax.rem(c + k, n_col)})

    def row_copy(p, s, q, k):
        return remote(part(p, s, d), row_send.at[q, k], row_recv.at[q], {"row": r + (1 if k else -1)})

    def depth_copy(p, s, q, held, bit):
        m = held | bit
        return remote(part(p, s, d ^ held if held else d), depth_send.at[q, m], depth_recv.at[q, m], {"depth": d ^ bit})

    chunks = [(p, s, p * PIECES + s) for p in range(PANELS) for s in range(PIECES)]
    for p, s, q in chunks:
        pl.when((r == p // n_col) & (c == p % n_col))(lambda p=p, s=s, q=q: local(p, s, q).start())

    def arrive(p, s, q):
        home, col = p // n_col, p % n_col

        @pl.when((r == home) & (c == col))
        def _():
            local(p, s, q).wait()
            for k in range(1, n_col):
                col_copy(p, s, q, k).start()

        @pl.when((r == home) & (c != col))
        def _():
            col_copy(p, s, q, 1).wait_recv()

        @pl.when(r != home)
        def _():
            row_copy(p, s, q, 0).wait_recv()

        pl.when((r <= home) & (r > 0))(lambda: row_copy(p, s, q, 0).start())
        pl.when((r >= home) & (r < n_row - 1))(lambda: row_copy(p, s, q, 1).start())
        if bits:
            depth_copy(p, s, q, 0, bits[0]).start()

    def level(p, s, q, t):
        held = [m for m in range(n_depth) if m % bits[t] == 0]
        for m in held:
            if m & bits[t]:
                depth_copy(p, s, q, m ^ bits[t], bits[t]).wait_recv()
        if t + 1 < len(bits):
            for m in held:
                depth_copy(p, s, q, m, bits[t + 1]).start()

    for n in range(len(chunks) + len(bits)):
        if n < len(chunks):
            arrive(*chunks[n])
        for t in range(len(bits)):
            if 0 <= n - 1 - t < len(chunks):
                level(*chunks[n - 1 - t], t)

    for p, s, q in chunks:
        home, col = p // n_col, p % n_col

        @pl.when((r == home) & (c == col))
        def _():
            for k in range(1, n_col):
                col_copy(p, s, q, k).wait_send()

        pl.when((r <= home) & (r > 0))(lambda: row_copy(p, s, q, 0).wait_send())
        pl.when((r >= home) & (r < n_row - 1))(lambda: row_copy(p, s, q, 1).wait_send())
        for t, bit in enumerate(bits):
            for m in range(n_depth):
                if m % (2 * bit) == 0:
                    depth_copy(p, s, q, m, bit).wait_send()


def collect(sizes, joined):
    n_row, n_col, n_depth = sizes
    rows_dev, width = joined.shape
    rank = width - PANELS * B
    count = PANELS * PIECES
    dma = pltpu.SemaphoreType.DMA
    hbm = pl.BlockSpec(memory_space=pl.ANY)
    return pl.pallas_call(
        functools.partial(send_kernel, sizes),
        out_shape=tuple(
            jax.ShapeDtypeStruct((n_depth, rows_dev, rank + (p + 1) * B), jnp.float32) for p in range(PANELS)
        ),
        in_specs=[pl.BlockSpec(memory_space=pltpu.VMEM)],
        out_specs=(hbm,) * PANELS,
        scratch_shapes=[
            dma((count,)),
            dma((count, n_col)),
            dma((count,)),
            dma((count, 2)),
            dma((count,)),
            dma((count, n_depth)),
            dma((count, n_depth)),
        ],
        compiler_params=pltpu.CompilerParams(collective_id=0, has_side_effects=True),
    )(joined)


def on_device(sizes, factor, update):
    rows_dev = factor.shape[0]
    row_start = lax.axis_index(("row", "col", "depth")) * rows_dev
    panel = jnp.minimum(row_start // B, PANELS - 1)
    start = jnp.stack([row_start, (panel + 1) * (B // T) - 1]).astype(jnp.int32)
    blocks = collect(sizes, jnp.concatenate([update, factor[:, : PANELS * B]], 1))
    slabs = [block.reshape(B, block.shape[2]) for block in blocks]
    return update_rows(start, slabs, factor, update)


def solution(mesh):
    sizes = tuple(mesh.shape[name] for name in ("row", "col", "depth"))
    return jax.shard_map(
        functools.partial(on_device, sizes),
        mesh=mesh,
        in_specs=(P(("row", "col", "depth"), None), P(("row", "col", "depth"), None)),
        out_specs=(P(("row", "col", "depth"), None), P(("row", "col", "depth"), None)),
        check_vma=False,
    )
```

```python
import functools

import jax
import jax.numpy as jnp
from jax import lax
from jax.experimental import pallas as pl
from jax.experimental.pallas import tpu as pltpu
from jax.sharding import PartitionSpec as P

B = 512
PANELS = 3
T = 128
PIECES = 4
MESH = pl.DeviceIdType.MESH
S = 16
NN = ((1,), (0,))
NT = ((1,), (1,))
TN = ((0,), (0,))


def split(x):
    high = x.astype(jnp.bfloat16)
    return high, (x - high.astype(jnp.float32)).astype(jnp.bfloat16)


def mms(a, b, dims):
    def dot(p, q):
        return lax.dot_general(p, q, (dims, ((), ())), preferred_element_type=jnp.float32)

    return dot(a[0], b[0]) + (dot(a[0], b[1]) + dot(a[1], b[0]))


def mm(a, b, dims):
    return mms(split(a), split(b), dims)


def invert(ref, count, symmetric):
    sub = lax.broadcasted_iota(jnp.int32, (S, T), 0)
    lane = lax.broadcasted_iota(jnp.int32, (S, T), 1)
    all_lane = lax.broadcasted_iota(jnp.int32, (T, T), 1)
    all_row = lax.broadcasted_iota(jnp.int32, (T, T), 0)

    def body(block, carry):
        first = pl.multiple_of(block * S, S)
        rows = [
            pltpu.roll(ref[m, pl.ds(first, S), :], lax.rem(T - first, T), 1) for m in range(count)
        ]
        diag = [jnp.ones((S, T), jnp.float32) for _ in range(count)]
        for s in range(S):
            for m in range(count):
                r = rows[m]
                col = jnp.broadcast_to(r[:, s : s + 1], (S, T))
                pivot = jnp.broadcast_to(col[s : s + 1, :], (S, T))
                diag[m] = jnp.where(sub == s, pivot, diag[m])
                r = jnp.where((lane == s) & (sub >= s), jnp.where(sub == s, 1.0, 0.0), r)
                scaled = r[s : s + 1, :] / pivot[0:1, :]
                rows[m] = r - jnp.where(sub > s, col, 0.0) * scaled
        in_block = (all_lane >= first) & (all_lane < first + S)
        for m in range(count):
            r = rows[m]
            r = r * lax.rsqrt(diag[m]) if symmetric else r / diag[m]
            r = pltpu.roll(r, first, 1)
            r = jnp.where((lane > sub + first) & (lane < first + S), 0.0, r)
            a = ref[m]
            right = split(r)
            if symmetric:
                left = split(jnp.where(lane >= first + S, r, 0.0))
                change = mms(left, right, TN)
                ref[m] = jnp.where(in_block, 0.0, a) - change
            else:
                left = jnp.where(in_block & (all_row >= first + S), a, 0.0)
                wide = [jnp.where(all_row // S == block, jnp.concatenate([q.astype(jnp.float32)] * (T // S), 0), 0.0).astype(jnp.bfloat16) for q in right]
                change = mms(split(left), wide, NN)
                ref[m] = jnp.where(in_block, 0.0, a) - change
            ref[m, pl.ds(first, S), :] = jnp.where(lane <= sub + first, r, 0.0)
        return carry

    lax.fori_loop(0, T // S, body, 0)


def kernel(start_ref, *refs):
    xs = refs[:PANELS]
    f_ref, u_ref, of_ref, ou_ref = refs[PANELS : PANELS + 4]
    w11, w22, w21, tinv_h, tinv_l, sinv, hh, hl, gh, gl = refs[PANELS + 4 :]
    per = B // T
    count = PANELS * per
    rank = u_ref.shape[1]
    half = rank // 2
    eye = jnp.where(
        lax.broadcasted_iota(jnp.int32, (T, T), 0) == lax.broadcasted_iota(jnp.int32, (T, T), 1), 1.0, 0.0
    )

    def blk(j):
        return slice(j * T, (j + 1) * T)

    total = [[eye, None], [jnp.zeros((half, half), jnp.float32), eye]]
    for j in range(count):
        t = xs[j // per][blk(j % per), :rank]
        if j:
            left = split(xs[j // per][blk(j % per), rank : rank + j * T])
            t = t - mms(left, (hh[: j * T, :], hl[: j * T, :]), NN)
        h = split(t)
        hh[blk(j), :], hl[blk(j), :] = h
        g = mms(h, h, TN)
        total[0][0] = total[0][0] + g[:half, :half]
        total[1][0] = total[1][0] + g[half:, :half]
        total[1][1] = total[1][1] + g[half:, half:]
        w11[j], w21[j], w22[j] = total[0][0], total[1][0], total[1][1]

    invert(w11, count, True)
    for j in range(count):
        low = mm(w21[j], w11[j], NT)
        w21[j] = low
        low = split(low)
        w22[j] = w22[j] - mms(low, low, NT)
    invert(w22, count, True)
    for j in range(count):
        x21 = -mm(w22[j], mm(w21[j], w11[j], NN), NN)
        for out, x11, x2, x22 in zip((tinv_h, tinv_l), split(w11[j]), split(x21), split(w22[j])):
            out[j, :half, :half] = x11
            out[j, :half, half:] = jnp.zeros_like(x11)
            out[j, half:, :half] = x2
            out[j, half:, half:] = x22
    for j in range(count):
        h = (hh[blk(j), :], hl[blk(j), :])
        g = h if j == 0 else split(mms(h, (tinv_h[j - 1], tinv_l[j - 1]), NT))
        gh[blk(j), :], gl[blk(j), :] = g
        sinv[j] = eye + mms(g, g, NT)
    invert(sinv, count, True)

    rows = f_ref.shape[0]
    row_ids = start_ref[0] + lax.broadcasted_iota(jnp.int32, (rows, T), 0)
    lane = lax.broadcasted_iota(jnp.int32, (rows, T), 1)
    res = u_ref[...]
    for j in range(count):
        f = f_ref[:, blk(j)]
        u = split(res)
        if j:
            u = split(mms(u, (tinv_h[j - 1], tinv_l[j - 1]), NT))
        z = f + mms(u, (gh[blk(j), :], gl[blk(j), :]), NT)
        y = mm(z, sinv[j], NT)
        of_ref[:, blk(j)] = jnp.where(row_ids >= lane + j * T, y, 0.0)
        res = res - mms(split(f), (hh[blk(j), :], hl[blk(j), :]), NN)
    last = start_ref[1]
    ou_ref[...] = mms(split(res), (tinv_h[last], tinv_l[last]), NT)


def solve_kernel(start_ref, f_ref, u_ref, out_ref, dinv):
    rank = u_ref.shape[1]
    width = out_ref.shape[1] - rank
    dinv[0] = f_ref[:, pl.ds(pl.multiple_of(start_ref[2] * T, T), T)]
    invert(dinv, 1, False)
    inverse = split(dinv[0])
    out_ref[:, :rank] = mms(inverse, split(u_ref[...]), NN)
    for k in range(0, width, T):
        out_ref[:, rank + k : rank + k + T] = mms(inverse, split(f_ref[:, k : k + T]), NN)


def solve_rows(start, factor, update):
    width = update.shape[1] + PANELS * B - T
    vmem = pl.BlockSpec(memory_space=pltpu.VMEM)
    return pl.pallas_call(
        solve_kernel,
        out_shape=jax.ShapeDtypeStruct((factor.shape[0], width), jnp.float32),
        in_specs=[pl.BlockSpec(memory_space=pltpu.SMEM), vmem, vmem],
        out_specs=vmem,
        scratch_shapes=[pltpu.VMEM((1, T, T), jnp.float32)],
    )(start, factor, update)


def update_rows(start, slabs, factor, update):
    count = PANELS * B // T
    rank = update.shape[1]
    half = rank // 2
    f32, b16 = jnp.float32, jnp.bfloat16
    vmem = pl.BlockSpec(memory_space=pltpu.VMEM)
    return pl.pallas_call(
        kernel,
        out_shape=(
            jax.ShapeDtypeStruct(factor.shape, f32),
            jax.ShapeDtypeStruct(update.shape, f32),
        ),
        in_specs=[pl.BlockSpec(memory_space=pltpu.SMEM)] + [vmem] * (PANELS + 2),
        out_specs=(vmem, vmem),
        scratch_shapes=[
            pltpu.VMEM((count, half, half), f32),
            pltpu.VMEM((count, half, half), f32),
            pltpu.VMEM((count, half, half), f32),
            pltpu.VMEM((count, rank, rank), b16),
            pltpu.VMEM((count, rank, rank), b16),
            pltpu.VMEM((count, T, T), f32),
            pltpu.VMEM((count * T, rank), b16),
            pltpu.VMEM((count * T, rank), b16),
            pltpu.VMEM((count * T, rank), b16),
            pltpu.VMEM((count * T, rank), b16),
        ],
        compiler_params=pltpu.CompilerParams(vmem_limit_bytes=56 * 1024 * 1024),
    )(start, *slabs, factor, update)


def send_kernel(sizes, x_ref, *refs):
    outs = refs[:PANELS]
    local_sem, col_send, col_recv, row_send, row_recv, depth_send, depth_recv = refs[PANELS:]
    n_row, n_col, n_depth = sizes
    r, c, d = (lax.axis_index(name) for name in ("row", "col", "depth"))
    bits = [1 << b for b in reversed(range(n_depth.bit_length() - 1))]
    rows_dev = x_ref.shape[0]
    piece = rows_dev // PIECES
    barrier = pltpu.get_barrier_semaphore()

    def greet(target):
        pl.semaphore_signal(barrier, inc=1, device_id=target, device_id_type=MESH)

    for k in range(1, n_col):
        greet({"col": lax.rem(c + k, n_col)})
    for bit in bits:
        greet({"depth": d ^ bit})
    turns = (1, n_row - 1) if n_row > 1 else ()
    for k in turns:
        greet({"row": lax.rem(r + k, n_row)})
    pl.semaphore_wait(barrier, n_col - 1 + len(bits) + len(turns))

    def part(p, s, owner):
        return outs[p].at[owner, pl.ds(s * piece, piece), :]

    def remote(ref, send, recv, target):
        return pltpu.make_async_remote_copy(
            src_ref=ref, dst_ref=ref, send_sem=send, recv_sem=recv, device_id=target, device_id_type=MESH
        )

    def local(p, s, q):
        width = outs[p].shape[2]
        return pltpu.make_async_copy(x_ref.at[pl.ds(s * piece, piece), :width], part(p, s, d), local_sem.at[q])

    def col_copy(p, s, q, k):
        return remote(part(p, s, d), col_send.at[q, k], col_recv.at[q], {"col": lax.rem(c + k, n_col)})

    def row_copy(p, s, q, k):
        return remote(part(p, s, d), row_send.at[q, k], row_recv.at[q], {"row": lax.rem(r + (1 if k else n_row - 1), n_row)})

    def depth_copy(p, s, q, held, bit):
        m = held | bit
        return remote(part(p, s, d ^ held if held else d), depth_send.at[q, m], depth_recv.at[q, m], {"depth": d ^ bit})

    def row_sends(p):
        home = p // n_col
        away = lax.rem(r - home + n_row, n_row)
        up = n_row // 2 if home % 2 else n_row - 1 - n_row // 2
        down = n_row - 1 - up
        sends_up = away < up
        sends_down = (away == 0) & (down > 0) | (away > n_row - down)
        return sends_down, sends_up

    chunks = [(p, s, p * PIECES + s) for p in range(PANELS) for s in range(PIECES)]
    for p, s, q in chunks:
        pl.when((r == p // n_col) & (c == p % n_col))(lambda p=p, s=s, q=q: local(p, s, q).start())

    def arrive(p, s, q):
        home, col = p // n_col, p % n_col

        @pl.when((r == home) & (c == col))
        def _():
            local(p, s, q).wait()
            for k in range(1, n_col):
                col_copy(p, s, q, k).start()

        @pl.when((r == home) & (c != col))
        def _():
            col_copy(p, s, q, 1).wait_recv()

        @pl.when(r != home)
        def _():
            row_copy(p, s, q, 0).wait_recv()

        for k, sends in enumerate(row_sends(p)):
            pl.when(sends)(lambda k=k: row_copy(p, s, q, k).start())
        if bits:
            depth_copy(p, s, q, 0, bits[0]).start()

    def level(p, s, q, t):
        held = [m for m in range(n_depth) if m % bits[t] == 0]
        for m in held:
            if m & bits[t]:
                depth_copy(p, s, q, m ^ bits[t], bits[t]).wait_recv()
        if t + 1 < len(bits):
            for m in held:
                depth_copy(p, s, q, m, bits[t + 1]).start()

    for n in range(len(chunks) + len(bits)):
        if n < len(chunks):
            arrive(*chunks[n])
        for t in range(len(bits)):
            if 0 <= n - 1 - t < len(chunks):
                level(*chunks[n - 1 - t], t)

    for p, s, q in chunks:
        home, col = p // n_col, p % n_col

        @pl.when((r == home) & (c == col))
        def _():
            for k in range(1, n_col):
                col_copy(p, s, q, k).wait_send()

        for k, sends in enumerate(row_sends(p)):
            pl.when(sends)(lambda k=k: row_copy(p, s, q, k).wait_send())
        for t, bit in enumerate(bits):
            for m in range(n_depth):
                if m % (2 * bit) == 0:
                    depth_copy(p, s, q, m, bit).wait_send()


def collect(sizes, joined):
    n_row, n_col, n_depth = sizes
    rows_dev, width = joined.shape
    rank = width - PANELS * B + T
    count = PANELS * PIECES
    dma = pltpu.SemaphoreType.DMA
    hbm = pl.BlockSpec(memory_space=pl.ANY)
    return pl.pallas_call(
        functools.partial(send_kernel, sizes),
        out_shape=tuple(
            jax.ShapeDtypeStruct((n_depth, rows_dev, rank + (p + 1) * B - T), jnp.float32) for p in range(PANELS)
        ),
        in_specs=[pl.BlockSpec(memory_space=pltpu.VMEM)],
        out_specs=(hbm,) * PANELS,
        scratch_shapes=[
            dma((count,)),
            dma((count, n_col)),
            dma((count,)),
            dma((count, 2)),
            dma((count,)),
            dma((count, n_depth)),
            dma((count, n_depth)),
        ],
        compiler_params=pltpu.CompilerParams(collective_id=0, has_side_effects=True),
    )(joined)


def on_device(sizes, factor, update):
    rows_dev = factor.shape[0]
    row_start = lax.axis_index(("row", "col", "depth")) * rows_dev
    panel = jnp.minimum(row_start // B, PANELS - 1)
    own = jnp.minimum(row_start // T, PANELS * B // T - 1)
    start = jnp.stack([row_start, (panel + 1) * (B // T) - 1, own]).astype(jnp.int32)
    blocks = collect(sizes, solve_rows(start, factor, update))
    slabs = [block.reshape(B, block.shape[2]) for block in blocks]
    return update_rows(start, slabs, factor, update)


def solution(mesh):
    sizes = tuple(mesh.shape[name] for name in ("row", "col", "depth"))
    return jax.shard_map(
        functools.partial(on_device, sizes),
        mesh=mesh,
        in_specs=(P(("row", "col", "depth"), None), P(("row", "col", "depth"), None)),
        out_specs=(P(("row", "col", "depth"), None), P(("row", "col", "depth"), None)),
        check_vma=False,
    )
```

```python
import functools

import jax
import jax.numpy as jnp
from jax import lax
from jax.experimental import pallas as pl
from jax.experimental.pallas import tpu as pltpu
from jax.sharding import PartitionSpec as P

B = 512
PANELS = 3
T = 128
PIECES = 4
MESH = pl.DeviceIdType.MESH
S = 16
NN = ((1,), (0,))
NT = ((1,), (1,))
TN = ((0,), (0,))


def split(x):
    high = x.astype(jnp.bfloat16)
    return high, (x - high.astype(jnp.float32)).astype(jnp.bfloat16)


def mms(a, b, dims):
    def dot(p, q):
        return lax.dot_general(p, q, (dims, ((), ())), preferred_element_type=jnp.float32)

    return dot(a[0], b[0]) + (dot(a[0], b[1]) + dot(a[1], b[0]))


def mm(a, b, dims):
    return mms(split(a), split(b), dims)


def invert(ref, count, symmetric):
    sub = lax.broadcasted_iota(jnp.int32, (S, T), 0)
    lane = lax.broadcasted_iota(jnp.int32, (S, T), 1)
    all_lane = lax.broadcasted_iota(jnp.int32, (T, T), 1)
    all_row = lax.broadcasted_iota(jnp.int32, (T, T), 0)

    def body(block, carry):
        first = pl.multiple_of(block * S, S)
        rows = [
            pltpu.roll(ref[m, pl.ds(first, S), :], lax.rem(T - first, T), 1) for m in range(count)
        ]
        diag = [jnp.ones((S, T), jnp.float32) for _ in range(count)]
        for s in range(S):
            for m in range(count):
                r = rows[m]
                col = jnp.broadcast_to(r[:, s : s + 1], (S, T))
                pivot = jnp.broadcast_to(col[s : s + 1, :], (S, T))
                diag[m] = jnp.where(sub == s, pivot, diag[m])
                r = jnp.where((lane == s) & (sub >= s), jnp.where(sub == s, 1.0, 0.0), r)
                scaled = r[s : s + 1, :] / pivot[0:1, :]
                rows[m] = r - jnp.where(sub > s, col, 0.0) * scaled
        in_block = (all_lane >= first) & (all_lane < first + S)
        for m in range(count):
            r = rows[m]
            r = r * lax.rsqrt(diag[m]) if symmetric else r / diag[m]
            r = pltpu.roll(r, first, 1)
            r = jnp.where((lane > sub + first) & (lane < first + S), 0.0, r)
            a = ref[m]
            right = split(r)
            if symmetric:
                left = split(jnp.where(lane >= first + S, r, 0.0))
                change = mms(left, right, TN)
                ref[m] = jnp.where(in_block, 0.0, a) - change
            else:
                left = jnp.where(in_block & (all_row >= first + S), a, 0.0)
                wide = [jnp.where(all_row // S == block, jnp.concatenate([q.astype(jnp.float32)] * (T // S), 0), 0.0).astype(jnp.bfloat16) for q in right]
                change = mms(split(left), wide, NN)
                ref[m] = jnp.where(in_block, 0.0, a) - change
            ref[m, pl.ds(first, S), :] = jnp.where(lane <= sub + first, r, 0.0)
        return carry

    lax.fori_loop(0, T // S, body, 0)


def kernel(start_ref, *refs):
    xs = refs[:PANELS]
    f_ref, u_ref, of_ref, ou_ref = refs[PANELS : PANELS + 4]
    w11, w22, w21, tinv_h, tinv_l, sinv, hh, hl, gh, gl = refs[PANELS + 4 :]
    per = B // T
    count = PANELS * per
    rank = u_ref.shape[1]
    half = rank // 2
    eye = jnp.where(
        lax.broadcasted_iota(jnp.int32, (T, T), 0) == lax.broadcasted_iota(jnp.int32, (T, T), 1), 1.0, 0.0
    )

    def blk(j):
        return slice(j * T, (j + 1) * T)

    total = [[eye, None], [jnp.zeros((half, half), jnp.float32), eye]]
    for j in range(count):
        t = xs[j // per][blk(j % per), :rank]
        if j:
            left = split(xs[j // per][blk(j % per), rank : rank + j * T])
            t = t - mms(left, (hh[: j * T, :], hl[: j * T, :]), NN)
        h = split(t)
        hh[blk(j), :], hl[blk(j), :] = h
        g = mms(h, h, TN)
        total[0][0] = total[0][0] + g[:half, :half]
        total[1][0] = total[1][0] + g[half:, :half]
        total[1][1] = total[1][1] + g[half:, half:]
        w11[j], w21[j], w22[j] = total[0][0], total[1][0], total[1][1]

    invert(w11, count, True)
    for j in range(count):
        low = mm(w21[j], w11[j], NT)
        w21[j] = low
        low = split(low)
        w22[j] = w22[j] - mms(low, low, NT)
    invert(w22, count, True)
    for j in range(count):
        x21 = -mm(w22[j], mm(w21[j], w11[j], NN), NN)
        for out, x11, x2, x22 in zip((tinv_h, tinv_l), split(w11[j]), split(x21), split(w22[j])):
            out[j, :half, :half] = x11
            out[j, :half, half:] = jnp.zeros_like(x11)
            out[j, half:, :half] = x2
            out[j, half:, half:] = x22
    for j in range(count):
        h = (hh[blk(j), :], hl[blk(j), :])
        g = h if j == 0 else split(mms(h, (tinv_h[j - 1], tinv_l[j - 1]), NT))
        gh[blk(j), :], gl[blk(j), :] = g
        sinv[j] = eye + mms(g, g, NT)
    invert(sinv, count, True)

    rows = f_ref.shape[0]
    row_ids = start_ref[0] + lax.broadcasted_iota(jnp.int32, (rows, T), 0)
    lane = lax.broadcasted_iota(jnp.int32, (rows, T), 1)
    res = u_ref[...]
    for j in range(count):
        f = f_ref[:, blk(j)]
        u = split(res)
        if j:
            u = split(mms(u, (tinv_h[j - 1], tinv_l[j - 1]), NT))
        z = f + mms(u, (gh[blk(j), :], gl[blk(j), :]), NT)
        y = mm(z, sinv[j], NT)
        of_ref[:, blk(j)] = jnp.where(row_ids >= lane + j * T, y, 0.0)
        res = res - mms(split(f), (hh[blk(j), :], hl[blk(j), :]), NN)
    last = start_ref[1]
    ou_ref[...] = mms(split(res), (tinv_h[last], tinv_l[last]), NT)


def solve_kernel(start_ref, f_ref, u_ref, out_ref, dinv):
    rank = u_ref.shape[1]
    width = out_ref.shape[1] - rank
    dinv[0] = f_ref[:, pl.ds(pl.multiple_of(start_ref[2] * T, T), T)]
    invert(dinv, 1, False)
    inverse = split(dinv[0])
    out_ref[:, :rank] = mms(inverse, split(u_ref[...]), NN)
    for k in range(0, width, T):
        out_ref[:, rank + k : rank + k + T] = mms(inverse, split(f_ref[:, k : k + T]), NN)


def solve_rows(start, factor, update):
    width = update.shape[1] + PANELS * B - T
    vmem = pl.BlockSpec(memory_space=pltpu.VMEM)
    return pl.pallas_call(
        solve_kernel,
        out_shape=jax.ShapeDtypeStruct((factor.shape[0], width), jnp.float32),
        in_specs=[pl.BlockSpec(memory_space=pltpu.SMEM), vmem, vmem],
        out_specs=vmem,
        scratch_shapes=[pltpu.VMEM((1, T, T), jnp.float32)],
    )(start, factor, update)


def update_rows(start, slabs, factor, update):
    count = PANELS * B // T
    rank = update.shape[1]
    half = rank // 2
    f32, b16 = jnp.float32, jnp.bfloat16
    vmem = pl.BlockSpec(memory_space=pltpu.VMEM)
    return pl.pallas_call(
        kernel,
        out_shape=(
            jax.ShapeDtypeStruct(factor.shape, f32),
            jax.ShapeDtypeStruct(update.shape, f32),
        ),
        in_specs=[pl.BlockSpec(memory_space=pltpu.SMEM)] + [vmem] * (PANELS + 2),
        out_specs=(vmem, vmem),
        scratch_shapes=[
            pltpu.VMEM((count, half, half), f32),
            pltpu.VMEM((count, half, half), f32),
            pltpu.VMEM((count, half, half), f32),
            pltpu.VMEM((count, rank, rank), b16),
            pltpu.VMEM((count, rank, rank), b16),
            pltpu.VMEM((count, T, T), f32),
            pltpu.VMEM((count * T, rank), b16),
            pltpu.VMEM((count * T, rank), b16),
            pltpu.VMEM((count * T, rank), b16),
            pltpu.VMEM((count * T, rank), b16),
        ],
        compiler_params=pltpu.CompilerParams(vmem_limit_bytes=56 * 1024 * 1024),
    )(start, *slabs, factor, update)


def send_kernel(sizes, x_ref, *refs):
    outs = refs[:PANELS]
    local_sem, col_send, col_recv, row_send, row_recv, depth_send, depth_recv = refs[PANELS:]
    n_row, n_col, n_depth = sizes
    r, c, d = (lax.axis_index(name) for name in ("row", "col", "depth"))
    bits = [1 << b for b in reversed(range(n_depth.bit_length() - 1))]
    rows_dev = x_ref.shape[0]
    piece = rows_dev // PIECES
    barrier = pltpu.get_barrier_semaphore()

    def greet(target):
        pl.semaphore_signal(barrier, inc=1, device_id=target, device_id_type=MESH)

    for k in range(1, n_col):
        greet({"col": lax.rem(c + k, n_col)})
    for bit in bits:
        greet({"depth": d ^ bit})
    turns = (1, n_row - 1) if n_row > 1 else ()
    for k in turns:
        greet({"row": lax.rem(r + k, n_row)})
    pl.semaphore_wait(barrier, n_col - 1 + len(bits) + len(turns))

    def part(p, s, owner):
        return outs[p].at[owner, pl.ds(s * piece, piece), :]

    def remote(ref, send, recv, target):
        return pltpu.make_async_remote_copy(
            src_ref=ref, dst_ref=ref, send_sem=send, recv_sem=recv, device_id=target, device_id_type=MESH
        )

    def local(p, s, q):
        width = outs[p].shape[2]
        return pltpu.make_async_copy(x_ref.at[pl.ds(s * piece, piece), :width], part(p, s, d), local_sem.at[q])

    def col_copy(p, s, q, k):
        return remote(part(p, s, d), col_send.at[q, k], col_recv.at[q], {"col": lax.rem(c + k, n_col)})

    def row_copy(p, s, q, k):
        return remote(part(p, s, d), row_send.at[q, k], row_recv.at[q], {"row": lax.rem(r + (1 if k else n_row - 1), n_row)})

    def depth_copy(p, s, q, held, bit):
        m = held | bit
        return remote(part(p, s, d ^ held if held else d), depth_send.at[q, m], depth_recv.at[q, m], {"depth": d ^ bit})

    def row_sends(p):
        home = p // n_col
        away = lax.rem(r - home + n_row, n_row)
        up = n_row - 1 - home
        down = n_row - 1 - up
        sends_up = away < up
        sends_down = (away == 0) & (down > 0) | (away > n_row - down)
        return sends_down, sends_up

    chunks = [(p, s, p * PIECES + s) for p in range(PANELS) for s in range(PIECES)]
    for p, s, q in chunks:
        pl.when((r == p // n_col) & (c == p % n_col))(lambda p=p, s=s, q=q: local(p, s, q).start())

    def arrive(p, s, q):
        home, col = p // n_col, p % n_col

        @pl.when((r == home) & (c == col))
        def _():
            local(p, s, q).wait()
            for k in range(1, n_col):
                col_copy(p, s, q, k).start()

        @pl.when((r == home) & (c != col))
        def _():
            col_copy(p, s, q, 1).wait_recv()

        @pl.when(r != home)
        def _():
            row_copy(p, s, q, 0).wait_recv()

        for k, sends in enumerate(row_sends(p)):
            pl.when(sends)(lambda k=k: row_copy(p, s, q, k).start())
        if bits:
            depth_copy(p, s, q, 0, bits[0]).start()

    def level(p, s, q, t):
        held = [m for m in range(n_depth) if m % bits[t] == 0]
        for m in held:
            if m & bits[t]:
                depth_copy(p, s, q, m ^ bits[t], bits[t]).wait_recv()
        if t + 1 < len(bits):
            for m in held:
                depth_copy(p, s, q, m, bits[t + 1]).start()

    for n in range(len(chunks) + len(bits)):
        if n < len(chunks):
            arrive(*chunks[n])
        for t in range(len(bits)):
            if 0 <= n - 1 - t < len(chunks):
                level(*chunks[n - 1 - t], t)

    for p, s, q in chunks:
        home, col = p // n_col, p % n_col

        @pl.when((r == home) & (c == col))
        def _():
            for k in range(1, n_col):
                col_copy(p, s, q, k).wait_send()

        for k, sends in enumerate(row_sends(p)):
            pl.when(sends)(lambda k=k: row_copy(p, s, q, k).wait_send())
        for t, bit in enumerate(bits):
            for m in range(n_depth):
                if m % (2 * bit) == 0:
                    depth_copy(p, s, q, m, bit).wait_send()


def collect(sizes, joined):
    n_row, n_col, n_depth = sizes
    rows_dev, width = joined.shape
    rank = width - PANELS * B + T
    count = PANELS * PIECES
    dma = pltpu.SemaphoreType.DMA
    hbm = pl.BlockSpec(memory_space=pl.ANY)
    return pl.pallas_call(
        functools.partial(send_kernel, sizes),
        out_shape=tuple(
            jax.ShapeDtypeStruct((n_depth, rows_dev, rank + (p + 1) * B - T), jnp.float32) for p in range(PANELS)
        ),
        in_specs=[pl.BlockSpec(memory_space=pltpu.VMEM)],
        out_specs=(hbm,) * PANELS,
        scratch_shapes=[
            dma((count,)),
            dma((count, n_col)),
            dma((count,)),
            dma((count, 2)),
            dma((count,)),
            dma((count, n_depth)),
            dma((count, n_depth)),
        ],
        compiler_params=pltpu.CompilerParams(collective_id=0, has_side_effects=True),
    )(joined)


def on_device(sizes, factor, update):
    rows_dev = factor.shape[0]
    row_start = lax.axis_index(("row", "col", "depth")) * rows_dev
    panel = jnp.minimum(row_start // B, PANELS - 1)
    own = jnp.minimum(row_start // T, PANELS * B // T - 1)
    start = jnp.stack([row_start, (panel + 1) * (B // T) - 1, own]).astype(jnp.int32)
    blocks = collect(sizes, solve_rows(start, factor, update))
    slabs = [block.reshape(B, block.shape[2]) for block in blocks]
    return update_rows(start, slabs, factor, update)


def solution(mesh):
    sizes = tuple(mesh.shape[name] for name in ("row", "col", "depth"))
    return jax.shard_map(
        functools.partial(on_device, sizes),
        mesh=mesh,
        in_specs=(P(("row", "col", "depth"), None), P(("row", "col", "depth"), None)),
        out_specs=(P(("row", "col", "depth"), None), P(("row", "col", "depth"), None)),
        check_vma=False,
    )
```
